32 devices in a mesh: expert: 2 (over y), shard: 16 (over z, x, core).
Axes of the slice: x: 2, y: 2, z: 4, core: 2. Of those that a mesh axis runs over, the one named last changes fastest.
Arguments:
- fast_weights: bfloat16 [2, 16, 1, 64, 14336], P('expert', 'shard'), may hold values from -0.125 to 0.125
- slow_weights: float32 [2, 1, 64, 14336], P('expert', None, None, 'shard'), may hold values from -0.09375 to 0.09375
- step_counts: int32 [2, 16], P('expert', 'shard'), may hold values from 1 to 16
- token_counts: int32 [2, 16], P('expert', 'shard'), may hold values from 100 to 897
Outputs:
- new_slow: float32 [2, 1, 64, 14336], P('expert', None, None, 'shard')
- reset_fast: bfloat16 [2, 1, 64, 14336], P('expert')
The draws below stay inside these ranges and needn't reach their ends.
All inputs are finite; a program needn't handle non-finite values.
Results may differ from the reference program's by a relative error of at most 0.001.
Values may be sent and summed in bfloat16 or wider, within the bound.
A program may use at most 64 MiB of HBM per device.

```python
import jax
import jax.numpy as jnp
from jax import lax

D = 4096
FF = 14336
LAYERS = 1
ROWS = 64
EXPERTS = 2
REPLICAS = 16


def draw_token_counts(key, part):
    base = jax.random.randint(key, (EXPERTS, REPLICAS), 100, 300)
    replica = jnp.arange(REPLICAS, dtype=jnp.int32)[None, :]
    return (base * (REPLICAS - 1 + 2 * replica) // (REPLICAS - 1)).astype(jnp.int32)


def place_ends(array, key, smallest, largest):
    longest = array.shape.index(max(array.shape))
    spots = []
    for shift in (0, 1):
        where = [jax.random.randint(jax.random.fold_in(key, axis), (), 0, length) for axis, length in enumerate(array.shape)]
        where[longest] = (where[longest] + shift) % array.shape[longest]
        spots.append(tuple(where))
    return array.at[spots[0]].set(smallest).at[spots[1]].set(largest)


def spiked(entries, own_key, source, target, blocks, factor):
    def block_of(position):
        return (jnp.arange(entries.shape[position]) // (entries.shape[position] // blocks)).reshape((-1,) + (1,) * (entries.ndim - 1 - position))

    near = jax.random.permutation(own_key, blocks)[block_of(target)]
    other_side = (block_of(target) + blocks // 2) % blocks
    return jnp.where((block_of(source) == near) | (block_of(source) == other_side), factor * entries, entries)


def steps_of(key, dims, pieces, smallest, top_value):
    def one(axis_at, blocks):
        draws = jax.random.uniform(jax.random.fold_in(jax.random.fold_in(key, 6), axis_at), (blocks,), jnp.float32, smallest / len(pieces), top_value / len(pieces))
        return jnp.repeat(jnp.exp(draws), dims[axis_at] // blocks).reshape((-1,) + (1,) * (len(dims) - axis_at - 1))

    loudness = one(*pieces[0])
    for cut in pieces[1:]:
        loudness = loudness * one(*cut)
    return loudness


def bell_draw(stream_key, shape, width, reach, shards=(), held_as=jnp.bfloat16):
    loudness = steps_of(stream_key, shape, shards, -0.22, 0.18) if shards else 1.0
    result = jax.random.normal(stream_key, shape, jnp.float32) * width * loudness
    return jnp.minimum(jnp.maximum(result, -reach), reach).astype(held_as)


def heavy_noise(stream_key, extent, width, reach, cuts, heavy, held_as=jnp.bfloat16):
    drawn = width * jax.random.normal(stream_key, extent, jnp.float32)
    if cuts:
        drawn = drawn * steps_of(stream_key, extent, cuts, -0.22, 0.18)
    return jnp.clip(spiked(drawn, jax.random.fold_in(stream_key, 3), *heavy), -reach, reach).astype(held_as)


def setup_inputs(seed: int = 0) -> dict:
    keys = jax.random.split(jax.random.key(seed), 5)
    return {
        "fast_weights": heavy_noise(keys[0], (EXPERTS, REPLICAS, LAYERS, ROWS, FF), D ** -0.5, 0.125, ((0, 2), (1, 16)), (1, 4, 16, 2.0)),
        "slow_weights": bell_draw(keys[1], (EXPERTS, LAYERS, ROWS, FF), D ** -0.5, 0.09375, ((0, 2), (3, 16)), jnp.float32),
        "step_counts": place_ends(jax.random.randint(keys[2], (EXPERTS, REPLICAS), 1, 17), jax.random.fold_in(keys[2], 1), 1, 16).astype(jnp.int32),
        "token_counts": draw_token_counts(jax.random.fold_in(keys[4], 71), 0),
    }


outer_rate = 0.7


def mix_one(args):
    fast, share = args
    return jnp.einsum("r,rlmn->lmn", share, fast.astype(jnp.float32), precision=lax.Precision.HIGHEST)


def reference(fast_weights, slow_weights, step_counts, token_counts):
    tokens = token_counts.astype(jnp.float32)
    steps = step_counts.astype(jnp.float32)
    share = tokens / steps
    tok = jnp.sum(tokens, axis=1)
    work = jnp.sum(tokens * steps, axis=1)
    qsum = jnp.sum(share, axis=1)
    total = jnp.sum(tok)
    mixed = lax.map(mix_one, (fast_weights, share))
    rate = outer_rate * EXPERTS * work / (tok * total)
    rate = rate[:, None, None, None]
    qsum = qsum[:, None, None, None]
    new_slow = slow_weights + rate * (mixed - qsum * slow_weights)
    return new_slow, new_slow.astype(jnp.bfloat16)
```

```python
import functools

import jax
import jax.numpy as jnp
from jax import lax
from jax.experimental import pallas as pl
from jax.experimental.pallas import tpu as pltpu
from jax.sharding import PartitionSpec as P

outer_rate = 0.7
MESH = pl.DeviceIdType.MESH
LANES = 128
PLANE = 4


def xor(inner, d):
    hi, lo = inner // 2, inner % 2
    return (hi + d // 2) % 2 * 2 + (lo + d % 2) % 2


def order_of(z, length):
    step = -1 if 2 * z < length - 1 else 1
    ts = [t for t in range(length)[::step] if t != z]
    return sorted(ts, key=lambda t: -abs(t - z))


def kernel(groups, length, pieces, fast, slow, steps, tokens, new_ref, full_ref,
           raw, left, right, outb, slow_v, stat, plane_stat, sems_s, sems_r, sem_l):
    rows, width = slow.shape
    part = rows // pieces
    e = lax.axis_index("expert")
    s = lax.axis_index("shard")
    z, inner = s // PLANE, s % PLANE

    def cols(t, i):
        return pl.ds(pl.multiple_of((t * PLANE + i) * width, LANES), width)

    def span(h):
        return pl.ds(h * part, part)

    barrier = pltpu.get_barrier_semaphore()
    peers = [((e + k) % groups, z * PLANE + xor(inner, d)) for k in range(groups) for d in range(PLANE) if k or d]
    peers += [(e, (z + k) % length * PLANE + inner) for k in range(1, length)]
    for peer in peers:
        pl.semaphore_signal(barrier, inc=1, device_id=peer, device_id_type=MESH)
    load_slow = pltpu.make_async_copy(slow, slow_v, sem_l.at[length])
    load_slow.start()
    own = [pltpu.make_async_copy(fast.at[:, cols(t, inner)], raw.at[0, t], sem_l.at[t]) for t in range(length)]
    for copy in own:
        copy.start()
    stat[0, 0:8, :] = jnp.full((8, LANES), tokens[0, 0].astype(jnp.float32))
    stat[0, 8:16, :] = jnp.full((8, LANES), steps[0, 0].astype(jnp.float32))
    pl.semaphore_wait(barrier, len(peers))

    def body(me):
        count = [0]
        sent = []

        def push(src, dst, recv, peer):
            copy = pltpu.make_async_remote_copy(
                src_ref=src, dst_ref=dst, send_sem=sems_s.at[count[0]], recv_sem=sems_r.at[recv],
                device_id=peer, device_id_type=MESH)
            count[0] += 1
            copy.start()
            sent.append(copy)

        def arrived(dst, recv):
            pltpu.make_async_remote_copy(
                src_ref=dst, dst_ref=dst, send_sem=sems_s.at[0], recv_sem=sems_r.at[recv],
                device_id=(e, s), device_id_type=MESH).wait_recv()

        base = 0
        r_raw = lambda d, t, h: ((d - 1) * length + t) * pieces + h
        base += (PLANE - 1) * length * pieces
        r_left = lambda t, h, b=base: b + t * pieces + h
        base += length * pieces
        r_right = lambda t, h, b=base: b + t * pieces + h
        base += length * pieces
        r_z = lambda t, h, b=base: b + t * pieces + h
        base += length * pieces
        r_x = lambda t, h, b=base: b + t * pieces + h
        base += length * pieces
        r_sib = lambda t, x, h, b=base: b + (t * 2 + x) * pieces + h
        base += 2 * length * pieces
        r_stat = lambda i, b=base: b + i
        base += groups * PLANE
        r_plane = lambda k, b=base: b + k

        at = lambda t, i: (e, t * PLANE + i)
        far = order_of(me, length)
        items = []
        for h in range(pieces):
            items += [(h, t) for t in far[:1]]
            if h:
                items.append((h - 1, me))
            items += [(h, t) for t in far[1:]]
        items.append((pieces - 1, me))

        for k in range(groups):
            for d in range(PLANE):
                if k or d:
                    i = (groups - k) % groups * PLANE + d
                    push(stat.at[0], stat.at[i], r_stat(i), ((e + k) % groups, me * PLANE + xor(inner, d)))
        for h, t in items:
            for d in (2, 3, 1):
                push(fast.at[span(h), cols(t, xor(inner, d))], raw.at[d, t, span(h)], r_raw(d, t, h), at(me, xor(inner, d)))

        def stats_in():
            for i in range(1, groups * PLANE):
                arrived(stat.at[i], r_stat(i))
            tok = [stat[i, 0:8, :] for i in range(groups * PLANE)]
            stp = [stat[i, 8:16, :] for i in range(groups * PLANE)]
            shares = [tok[i] / stp[i] for i in range(PLANE)]
            plane_stat[0, 0:8, :] = sum(tok[:PLANE])
            plane_stat[0, 8:16, :] = sum(tok[i] * stp[i] for i in range(PLANE))
            plane_stat[0, 16:24, :] = sum(shares)
            plane_stat[0, 24:32, :] = sum(tok)
            return [v[0:1, 0:1] for v in shares]

        shares = stats_in()
        for copy in own:
            copy.wait()

        def finish(h, first):
            if first:
                load_slow.wait()
                for k in range(1, length):
                    arrived(plane_stat.at[k], r_plane(k))
            tok, work, qsum, total = (
                sum(plane_stat[k, 8 * j:8 * j + 8, :] for k in range(length))[0:1, 0:1] for j in range(4))
            rate = outer_rate * groups * work / (tok * total)
            return rate, qsum

        def spread(t, h):
            ref = full_ref.at[span(h), cols(t, inner)]
            push(ref, ref, r_x(t, h), at(me, xor(inner, 2)))
            push(ref, ref, r_sib(t, 0, h), at(me, xor(inner, 1)))

        def from_z(h):
            for t in sorted((t for t in range(length) if t != me), key=lambda t: abs(t - me)):
                arrived(full_ref.at[span(h), cols(t, inner)], r_z(t, h))
                spread(t, h)

        def from_x(h):
            for t in sorted(range(length), key=lambda t: abs(t - me)):
                i = xor(inner, 2)
                ref = full_ref.at[span(h), cols(t, i)]
                arrived(ref, r_x(t, h))
                push(ref, ref, r_sib(t, 1, h), at(me, xor(inner, 1)))

        for n, (h, t) in enumerate(items):
            for d in range(1, PLANE):
                arrived(raw.at[d, t, span(h)], r_raw(d, t, h))
            came = []
            if t >= me and me > 0:
                arrived(left.at[t, span(h)], r_left(t, h))
                came.append(left)
            if t <= me and me < length - 1:
                arrived(right.at[t, span(h)], r_right(t, h))
                came.append(right)
            if t == me:
                rate, qsum = finish(h, h == 0)
            for r0 in range(h * part, (h + 1) * part, 16):
                sl = pl.ds(r0, 16)
                acc = shares[0] * raw[0, t, sl, :].astype(jnp.float32)
                for d in range(1, PLANE):
                    acc += shares[d] * raw[d, t, sl, :].astype(jnp.float32)
                for ref in came:
                    acc += ref[t, sl, :]
                if t == me:
                    old = slow_v[sl, :]
                    new = old + rate * (acc - qsum * old)
                    new_ref[sl, :] = new
                    full_ref[sl, cols(me, inner)] = new.astype(jnp.bfloat16)
                else:
                    outb[t, sl, :] = acc
            if t == me:
                ref = full_ref.at[span(h), cols(me, inner)]
                for other in order_of(me, length):
                    push(ref, ref, r_z(me, h), at(other, inner))
                spread(me, h)
            elif t > me:
                push(outb.at[t, span(h)], left.at[t, span(h)], r_left(t, h), at(me + 1, inner))
            else:
                push(outb.at[t, span(h)], right.at[t, span(h)], r_right(t, h), at(me - 1, inner))
            if n == 0:
                for k in range(1, length):
                    j = length - k
                    push(plane_stat.at[0], plane_stat.at[j], r_plane(j), at((me + k) % length, inner))
            if n == len(items) - 2:
                for g in range(pieces - 1):
                    from_z(g)
        from_z(pieces - 1)
        for h in range(pieces):
            from_x(h)
        for h in range(pieces):
            for t in range(length):
                arrived(full_ref.at[span(h), cols(t, xor(inner, 1))], r_sib(t, 0, h))
                arrived(full_ref.at[span(h), cols(t, xor(inner, 3))], r_sib(t, 1, h))
        for copy in sent:
            copy.wait_send()

    for me in range(length):
        pl.when(z == me)(functools.partial(body, me))


def shards_kernel(groups, devices, fast_weights, slow_weights, step_counts, token_counts):
    rows, full = fast_weights.shape[-2:]
    width = slow_weights.shape[-1]
    length = devices // PLANE
    pieces = 2
    sems = length * pieces * (PLANE - 1 + 6) + groups * PLANE + length + 8
    new, reset = pl.pallas_call(
        functools.partial(kernel, groups, length, pieces),
        out_shape=(jax.ShapeDtypeStruct((rows, width), jnp.float32), jax.ShapeDtypeStruct((rows, full), jnp.bfloat16)),
        in_specs=[pl.BlockSpec(memory_space=pl.ANY)] * 2 + [pl.BlockSpec(memory_space=pltpu.SMEM)] * 2,
        out_specs=(pl.BlockSpec(memory_space=pltpu.VMEM),) * 2,
        scratch_shapes=[
            pltpu.VMEM((PLANE, length, rows, width), jnp.bfloat16),
            pltpu.VMEM((length, rows, width), jnp.float32),
            pltpu.VMEM((length, rows, width), jnp.float32),
            pltpu.VMEM((length, rows, width), jnp.float32),
            pltpu.VMEM((rows, width), jnp.float32),
            pltpu.VMEM((groups * PLANE, 16, LANES), jnp.float32),
            pltpu.VMEM((length, 32, LANES), jnp.float32),
            pltpu.SemaphoreType.DMA((sems,)),
            pltpu.SemaphoreType.DMA((sems,)),
            pltpu.SemaphoreType.DMA((length + 1,)),
        ],
        compiler_params=pltpu.CompilerParams(collective_id=0, has_side_effects=True),
    )(fast_weights[0, 0, 0], slow_weights[0, 0], step_counts, token_counts)
    return new[None, None], reset[None, None]


def shards_plain(fast_weights, slow_weights, step_counts, token_counts):
    tokens = token_counts.astype(jnp.float32)[0, 0]
    steps = step_counts.astype(jnp.float32)[0, 0]
    share = tokens / steps
    work = tokens * steps
    groups = lax.axis_size("expert")
    tok_e, work_e, qsum = lax.psum((tokens, work, share), "shard")
    total = lax.psum(tok_e, "expert")
    rate = outer_rate * groups * work_e / (tok_e * total)
    weighted = share * fast_weights[0, 0].astype(jnp.float32)
    slow_part = slow_weights[0]
    mixed = lax.psum_scatter(weighted, "shard", scatter_dimension=2, tiled=True)
    new_slow = slow_part + rate * (mixed - qsum * slow_part)
    reset = lax.all_gather(new_slow.astype(jnp.bfloat16), "shard", axis=2, tiled=True)
    return (new_slow[None], reset[None])


def solution(mesh):
    groups, devices = mesh.shape["expert"], mesh.shape["shard"]

    def step(fast_weights, slow_weights, step_counts, token_counts):
        layers, rows, width = slow_weights.shape[1:]
        whole = devices % PLANE == 0 and devices > PLANE and rows % 32 == 0 and width % LANES == 0
        if whole and layers == 1:
            return shards_kernel(groups, devices, fast_weights, slow_weights, step_counts, token_counts)
        return shards_plain(fast_weights, slow_weights, step_counts, token_counts)

    placed = (
        P("expert", "shard", None, None, None),
        P("expert", None, None, "shard"),
        P("expert", "shard"),
        P("expert", "shard"),
    )
    return jax.shard_map(
        step,
        mesh=mesh,
        in_specs=placed,
        out_specs=(P("expert", None, None, "shard"), P("expert", None, None, None)),
        check_vma=False,
    )
```

```python
import functools

import jax
import jax.numpy as jnp
from jax import lax
from jax.experimental import pallas as pl
from jax.experimental.pallas import tpu as pltpu
from jax.sharding import PartitionSpec as P

outer_rate = 0.7
MESH = pl.DeviceIdType.MESH
LANES = 128
PLANE = 4


def xor(inner, d):
    hi, lo = inner // 2, inner % 2
    return (hi + d // 2) % 2 * 2 + (lo + d % 2) % 2


def order_of(z, length):
    step = -1 if 2 * z < length - 1 else 1
    ts = [t for t in range(length)[::step] if t != z]
    return sorted(ts, key=lambda t: -abs(t - z))


def PLAN(far, me, pieces, lag=4, zlag=8):
    plan, owned, passed = [], 0, 0
    sums = [(h, t) for h in range(pieces) for t in far]
    for n in range(len(sums) + max(lag, zlag) + 1):
        if owned < pieces and n >= (owned + 1) * len(far) + lag or (n >= len(sums) and owned < pieces):
            plan.append(("r", owned, me))
            owned += 1
        if passed < owned and n >= (passed + 1) * len(far) + zlag:
            plan.append(("z", passed, me))
            passed += 1
        if n < len(sums):
            plan.append(("r", *sums[n]))
    plan += [("r", h, me) for h in range(owned, pieces)]
    plan += [("z", h, me) for h in range(passed, pieces)]
    plan += [("x", h, me) for h in range(pieces)]
    feed = [(h, t) for what, h, t in plan if what == "r"]
    return feed, plan


def kernel(groups, length, bounds, fast, slow, steps, tokens, new_ref, full_ref,
           raw, left, right, outb, slow_v, stat, plane_stat, sems_s, sems_r, sem_l):
    rows, width = slow.shape
    pieces = len(bounds) - 1
    e = lax.axis_index("expert")
    s = lax.axis_index("shard")
    z, inner = s // PLANE, s % PLANE

    def cols(t, i):
        return pl.ds(pl.multiple_of((t * PLANE + i) * width, LANES), width)

    def span(h):
        return pl.ds(bounds[h], bounds[h + 1] - bounds[h])

    barrier = pltpu.get_barrier_semaphore()
    peers = [((e + k) % groups, z * PLANE + xor(inner, d)) for k in range(groups) for d in range(PLANE) if k or d]
    peers += [(e, (z + k) % length * PLANE + inner) for k in range(1, length)]
    for peer in peers:
        pl.semaphore_signal(barrier, inc=1, device_id=peer, device_id_type=MESH)
    load_slow = pltpu.make_async_copy(slow, slow_v, sem_l.at[length])
    load_slow.start()
    own = [pltpu.make_async_copy(fast.at[:, cols(t, inner)], raw.at[0, t], sem_l.at[t]) for t in range(length)]
    for copy in own:
        copy.start()
    stat[0, 0:8, :] = jnp.full((8, LANES), tokens[0, 0].astype(jnp.float32))
    stat[0, 8:16, :] = jnp.full((8, LANES), steps[0, 0].astype(jnp.float32))
    pl.semaphore_wait(barrier, len(peers))

    def body(me):
        count = [0]
        sent = []

        def push(src, dst, recv, peer):
            copy = pltpu.make_async_remote_copy(
                src_ref=src, dst_ref=dst, send_sem=sems_s.at[count[0]], recv_sem=sems_r.at[recv],
                device_id=peer, device_id_type=MESH)
            count[0] += 1
            copy.start()
            sent.append(copy)

        def arrived(dst, recv):
            pltpu.make_async_remote_copy(
                src_ref=dst, dst_ref=dst, send_sem=sems_s.at[0], recv_sem=sems_r.at[recv],
                device_id=(e, s), device_id_type=MESH).wait_recv()

        base = 0
        r_raw = lambda d, t, h: ((d - 1) * length + t) * pieces + h
        base += (PLANE - 1) * length * pieces
        r_left = lambda t, h, b=base: b + t * pieces + h
        base += length * pieces
        r_right = lambda t, h, b=base: b + t * pieces + h
        base += length * pieces
        r_z = lambda t, h, b=base: b + t * pieces + h
        base += length * pieces
        r_x = lambda t, h, b=base: b + t * pieces + h
        base += length * pieces
        r_sib = lambda t, x, h, b=base: b + (t * 2 + x) * pieces + h
        base += 2 * length * pieces
        r_stat = lambda i, b=base: b + i
        base += groups * PLANE
        r_plane = lambda k, b=base: b + k

        at = lambda t, i: (e, t * PLANE + i)
        far = order_of(me, length)
        feed, plan = PLAN(far, me, pieces)

        for k in range(groups):
            for d in range(PLANE):
                if k or d:
                    i = (groups - k) % groups * PLANE + d
                    push(stat.at[0], stat.at[i], r_stat(i), ((e + k) % groups, me * PLANE + xor(inner, d)))
        def give(n):
            h, t = feed[n]
            for d in (2, 3, 1):
                push(fast.at[span(h), cols(t, xor(inner, d))], raw.at[d, t, span(h)], r_raw(d, t, h), at(me, xor(inner, d)))

        for n in range(min(8, len(feed))):
            give(n)
        given = [min(8, len(feed))]

        def stats_in():
            for i in range(1, groups * PLANE):
                arrived(stat.at[i], r_stat(i))
            tok = [stat[i, 0:8, :] for i in range(groups * PLANE)]
            stp = [stat[i, 8:16, :] for i in range(groups * PLANE)]
            shares = [tok[i] / stp[i] for i in range(PLANE)]
            plane_stat[0, 0:8, :] = sum(tok[:PLANE])
            plane_stat[0, 8:16, :] = sum(tok[i] * stp[i] for i in range(PLANE))
            plane_stat[0, 16:24, :] = sum(shares)
            plane_stat[0, 24:32, :] = sum(tok)
            return [v[0:1, 0:1] for v in shares]

        shares = stats_in()
        for copy in own:
            copy.wait()

        def finish(h, first):
            if first:
                load_slow.wait()
                for k in range(1, length):
                    arrived(plane_stat.at[k], r_plane(k))
            tok, work, qsum, total = (
                sum(plane_stat[k, 8 * j:8 * j + 8, :] for k in range(length))[0:1, 0:1] for j in range(4))
            rate = outer_rate * groups * work / (tok * total)
            return rate, qsum

        def spread(t, h):
            ref = full_ref.at[span(h), cols(t, inner)]
            push(ref, ref, r_x(t, h), at(me, xor(inner, 2)))
            push(ref, ref, r_sib(t, 0, h), at(me, xor(inner, 1)))

        def from_z(h):
            for t in sorted((t for t in range(length) if t != me), key=lambda t: abs(t - me)):
                arrived(full_ref.at[span(h), cols(t, inner)], r_z(t, h))
                spread(t, h)

        def from_x(h):
            for t in sorted(range(length), key=lambda t: abs(t - me)):
                i = xor(inner, 2)
                ref = full_ref.at[span(h), cols(t, i)]
                arrived(ref, r_x(t, h))
                push(ref, ref, r_sib(t, 1, h), at(me, xor(inner, 1)))

        for n, (what, h, t) in enumerate(plan):
            if what == "z":
                from_z(h)
                continue
            if what == "x":
                from_x(h)
                continue
            for d in range(1, PLANE):
                arrived(raw.at[d, t, span(h)], r_raw(d, t, h))
            if given[0] < len(feed):
                give(given[0])
                given[0] += 1
            came = []
            if t >= me and me > 0:
                arrived(left.at[t, span(h)], r_left(t, h))
                came.append(left)
            if t <= me and me < length - 1:
                arrived(right.at[t, span(h)], r_right(t, h))
                came.append(right)
            if t == me:
                rate, qsum = finish(h, h == 0)
            for r0 in range(bounds[h], bounds[h + 1], 16):
                sl = pl.ds(r0, 16)
                acc = shares[0] * raw[0, t, sl, :].astype(jnp.float32)
                for d in range(1, PLANE):
                    acc += shares[d] * raw[d, t, sl, :].astype(jnp.float32)
                for ref in came:
                    acc += ref[t, sl, :]
                if t == me:
                    old = slow_v[sl, :]
                    new = old + rate * (acc - qsum * old)
                    new_ref[sl, :] = new
                    full_ref[sl, cols(me, inner)] = new.astype(jnp.bfloat16)
                else:
                    outb[t, sl, :] = acc
            if t == me:
                ref = full_ref.at[span(h), cols(me, inner)]
                for other in order_of(me, length):
                    push(ref, ref, r_z(me, h), at(other, inner))
                spread(me, h)
            elif t > me:
                push(outb.at[t, span(h)], left.at[t, span(h)], r_left(t, h), at(me + 1, inner))
            else:
                push(outb.at[t, span(h)], right.at[t, span(h)], r_right(t, h), at(me - 1, inner))
            if n == 0:
                for k in range(1, length):
                    j = length - k
                    push(plane_stat.at[0], plane_stat.at[j], r_plane(j), at((me + k) % length, inner))
        for h in range(pieces):
            for t in range(length):
                arrived(full_ref.at[span(h), cols(t, xor(inner, 1))], r_sib(t, 0, h))
                arrived(full_ref.at[span(h), cols(t, xor(inner, 3))], r_sib(t, 1, h))
        for copy in sent:
            copy.wait_send()

    for me in range(length):
        pl.when(z == me)(functools.partial(body, me))


def shards_kernel(groups, devices, fast_weights, slow_weights, step_counts, token_counts):
    rows, full = fast_weights.shape[-2:]
    width = slow_weights.shape[-1]
    length = devices // PLANE
    bounds = tuple(range(0, rows + 1, max(rows // 64, 1) * 16))
    pieces = len(bounds) - 1
    sems = length * pieces * (PLANE - 1 + 6) + groups * PLANE + length + 8
    new, reset = pl.pallas_call(
        functools.partial(kernel, groups, length, bounds),
        out_shape=(pltpu.VMEM((rows, width), jnp.float32), pltpu.VMEM((rows, full), jnp.bfloat16)),
        in_specs=[pl.BlockSpec(memory_space=pl.ANY)] * 2 + [pl.BlockSpec(memory_space=pltpu.SMEM)] * 2,
        out_specs=(pl.BlockSpec(memory_space=pltpu.VMEM),) * 2,
        scratch_shapes=[
            pltpu.VMEM((PLANE, length, rows, width), jnp.bfloat16),
            pltpu.VMEM((length, rows, width), jnp.float32),
            pltpu.VMEM((length, rows, width), jnp.float32),
            pltpu.VMEM((length, rows, width), jnp.float32),
            pltpu.VMEM((rows, width), jnp.float32),
            pltpu.VMEM((groups * PLANE, 16, LANES), jnp.float32),
            pltpu.VMEM((length, 32, LANES), jnp.float32),
            pltpu.SemaphoreType.DMA((sems,)),
            pltpu.SemaphoreType.DMA((sems,)),
            pltpu.SemaphoreType.DMA((length + 1,)),
        ],
        compiler_params=pltpu.CompilerParams(collective_id=0, has_side_effects=True),
    )(fast_weights[0, 0, 0], slow_weights[0, 0], step_counts, token_counts)
    return new[None, None], reset[None, None]


def shards_plain(fast_weights, slow_weights, step_counts, token_counts):
    tokens = token_counts.astype(jnp.float32)[0, 0]
    steps = step_counts.astype(jnp.float32)[0, 0]
    share = tokens / steps
    work = tokens * steps
    groups = lax.axis_size("expert")
    tok_e, work_e, qsum = lax.psum((tokens, work, share), "shard")
    total = lax.psum(tok_e, "expert")
    rate = outer_rate * groups * work_e / (tok_e * total)
    weighted = share * fast_weights[0, 0].astype(jnp.float32)
    slow_part = slow_weights[0]
    mixed = lax.psum_scatter(weighted, "shard", scatter_dimension=2, tiled=True)
    new_slow = slow_part + rate * (mixed - qsum * slow_part)
    reset = lax.all_gather(new_slow.astype(jnp.bfloat16), "shard", axis=2, tiled=True)
    return (new_slow[None], reset[None])


def solution(mesh):
    groups, devices = mesh.shape["expert"], mesh.shape["shard"]

    def step(fast_weights, slow_weights, step_counts, token_counts):
        layers, rows, width = slow_weights.shape[1:]
        whole = devices % PLANE == 0 and devices > PLANE and rows % 64 == 0 and width % LANES == 0
        if whole and layers == 1:
            return shards_kernel(groups, devices, fast_weights, slow_weights, step_counts, token_counts)
        return shards_plain(fast_weights, slow_weights, step_counts, token_counts)

    placed = (
        P("expert", "shard", None, None, None),
        P("expert", None, None, "shard"),
        P("expert", "shard"),
        P("expert", "shard"),
    )
    return jax.shard_map(
        step,
        mesh=mesh,
        in_specs=placed,
        out_specs=(P("expert", None, None, "shard"), P("expert", None, None, None)),
        check_vma=False,
    )
```
